32 devices in a mesh: dp: 4 (over y, x), tensor: 8 (over z, core).
Axes of the slice: x: 2, y: 2, z: 4, core: 2. Of those that a mesh axis runs over, the one named last changes fastest.
Arguments:
- saved_input: bfloat16 [512, 8192], P(('dp', 'tensor')), may hold values from -8 to 8
- keep_bits: int32 [512, 448], P(('dp', 'tensor')), may hold values from -2147483648 to 2147483646, as said below
- norm_gain: bfloat16 [8192], P('dp'), may hold values from 0.099609375 to 1.8984375
- gate_weight: bfloat16 [8192, 14336], P('dp', 'tensor'), may hold values from -0.0625 to 0.0625
- up_weight: bfloat16 [8192, 14336], P('dp', 'tensor'), may hold values from -0.0625 to 0.0625
- down_weight: bfloat16 [14336, 8192], P('tensor', 'dp'), may hold values from -0.046875 to 0.046875
Outputs:
- layer_out: bfloat16 [512, 8192], P('tensor', 'dp')
- row_check: float32 [512], P('tensor')
The draws below stay inside these ranges and needn't reach their ends.
Inputs may be any that keep to these rules, and one draw needn't show every extreme that they name: `keep_bits`: bit k of word w of a token is the keep bit of hidden unit 32 w + k.
All inputs are finite; a program needn't handle non-finite values.
Results may differ from the reference program's by a relative error of at most 0.017.
Values may be sent and summed in bfloat16 or wider, within the bound.
A program may use at most 64 MiB of HBM per device.

```python
import jax
import jax.numpy as jnp
from jax import lax

D = 8192
FF = 14336
TOKENS = 512
WORDS = 448


def draw_saved_input(key, part):
    keys = jax.random.split(jax.random.fold_in(key, 11), 2)
    base = jax.random.normal(keys[0], (TOKENS, D), jnp.float32)
    rough = jnp.exp(jax.random.uniform(keys[1], (1, D), jnp.float32, -0.35, 0.35))
    rising = jnp.exp(jnp.linspace(-0.55, 0.55, D, dtype=jnp.float32))[None, :]
    values = base * rough * rising
    return jnp.clip(values, -8.0, 8.0).astype(jnp.bfloat16)


def draw_keep_bits(key, part):
    return jax.random.randint(jax.random.fold_in(key, 23), (TOKENS, WORDS), -2147483648, 2147483647, jnp.int32)


def block_levels(own_key, shape, shards, low, high):
    def one(dim, parts):
        heights = jax.random.uniform(jax.random.fold_in(jax.random.fold_in(own_key, 6), dim), (parts,), jnp.float32, low / len(shards), high / len(shards))
        return jnp.repeat(jnp.exp(heights), shape[dim] // parts).reshape((-1,) + (1,) * (len(shape) - dim - 1))

    gain = one(*shards[0])
    for cut in shards[1:]:
        gain = gain * one(*cut)
    return gain


def scatter_about(stream_key, dims, deviation, most, cuts=(), kind=jnp.bfloat16):
    level = block_levels(stream_key, dims, cuts, -0.22, 0.18) if cuts else 1.0
    result = jax.random.normal(stream_key, dims, jnp.float32) * deviation * level
    return jnp.minimum(jnp.maximum(result, -most), most).astype(kind)


def setup_inputs(seed: int = 0) -> dict:
    arg_keys = jax.random.split(jax.random.key(seed), 7)
    return {
        "saved_input": draw_saved_input(jax.random.fold_in(arg_keys[6], 71), 0),
        "keep_bits": draw_keep_bits(jax.random.fold_in(arg_keys[6], 71), 0),
        "norm_gain": jnp.clip(1.0 + 0.18 * jax.random.normal(arg_keys[2], (D,), jnp.float32), 0.099609375, 1.8984375).astype(jnp.bfloat16),
        "gate_weight": scatter_about(arg_keys[3], (D, FF), D ** -0.5, 0.0625, ((0, 4), (1, 8))),
        "up_weight": scatter_about(arg_keys[4], (D, FF), D ** -0.5, 0.0625, ((0, 4), (1, 8))),
        "down_weight": scatter_about(arg_keys[5], (FF, D), FF ** -0.5, 0.046875, ((0, 8), (1, 4))),
    }


def reference(saved_input, keep_bits, norm_gain, gate_weight, up_weight, down_weight):
    widened = saved_input.astype(jnp.float32)
    inv_rms = lax.rsqrt(lax.optimization_barrier(jnp.sum(widened * widened, axis=1, keepdims=True)) / D + 1e-05)
    normed = (widened * inv_rms * norm_gain.astype(jnp.float32)).astype(jnp.bfloat16)
    gate = jnp.dot(normed, gate_weight, preferred_element_type=jnp.float32)
    up_sum = jnp.dot(normed, up_weight, preferred_element_type=jnp.float32)
    shifts = jnp.arange(32, dtype=jnp.int32)
    keep_mask = jnp.bitwise_and(jnp.right_shift(keep_bits[:, :, None], shifts[None, None, :]), 1)
    keep_mask = keep_mask.reshape(keep_bits.shape[0], -1)
    hidden = (jax.nn.silu(gate) * up_sum * (2.0 * keep_mask.astype(jnp.float32))).astype(jnp.bfloat16)
    layer_out = (widened + jnp.dot(hidden, down_weight, preferred_element_type=jnp.float32)).astype(jnp.bfloat16)
    widened_out = layer_out.astype(jnp.float32)
    row_check = lax.optimization_barrier(jnp.sum(widened_out * widened_out, axis=1)) / D
    return (layer_out, row_check)
```

```python
import jax
import jax.numpy as jnp
from jax import lax
from jax.experimental import pallas as pl
from jax.experimental.pallas import tpu as pltpu
from jax.sharding import PartitionSpec as P

D = 8192


def on_device(saved_input, keep_bits, norm_gain, gate_weight, up_weight, down_weight):
    tensor_width = lax.axis_size("tensor")
    dp_width = lax.axis_size("dp")
    unit_words = lax.all_to_all(keep_bits, "tensor", split_axis=1, concat_axis=0, tiled=True)
    shifts = jnp.arange(32, dtype=jnp.int32)
    keep_mask = jnp.bitwise_and(jnp.right_shift(unit_words[:, :, None], shifts[None, None, :]), 1)
    keep_mask = keep_mask.reshape(unit_words.shape[0], -1)
    keep_scale = 2.0 * keep_mask.astype(jnp.float32)
    width_units = gate_weight.shape[1]
    columns = lax.all_to_all(saved_input, "dp", split_axis=1, concat_axis=0, tiled=True)
    collected = lax.all_gather(columns, "tensor", axis=0, tiled=True)
    per_device = saved_input.shape[0]
    collected = collected.reshape(tensor_width, dp_width, per_device, collected.shape[1])
    collected = collected.transpose(1, 0, 2, 3).reshape(-1, collected.shape[3])
    widened = collected.astype(jnp.float32)
    squares = lax.psum(jnp.sum(widened * widened, axis=1), "dp")
    inv_rms = lax.rsqrt(squares / D + 1e-05)
    normed = (widened * inv_rms[:, None] * norm_gain.astype(jnp.float32)[None, :]).astype(
        jnp.bfloat16
    )
    gate_part = jnp.dot(normed, gate_weight, preferred_element_type=jnp.float32)
    up_part = jnp.dot(normed, up_weight, preferred_element_type=jnp.float32)
    projected = lax.psum_scatter(
        jnp.concatenate((gate_part, up_part), axis=1).astype(jnp.bfloat16),
        "dp",
        scatter_dimension=0,
        tiled=True,
    ).astype(jnp.float32)
    gate_sum = projected[:, :width_units]
    up_sum = projected[:, width_units:]
    hidden = (jax.nn.silu(gate_sum) * up_sum * keep_scale).astype(jnp.bfloat16)
    partial_value = jnp.dot(
        lax.all_gather(hidden, "dp", axis=0, tiled=True),
        down_weight,
        preferred_element_type=jnp.float32,
    )
    mlp_sum = lax.psum_scatter(
        partial_value.astype(jnp.bfloat16), "tensor", scatter_dimension=0, tiled=True
    ).astype(jnp.float32)
    out_rows = mlp_sum.shape[0]
    first_row = lax.axis_index("tensor") * out_rows
    residual = lax.dynamic_slice_in_dim(collected, first_row, out_rows, 0)
    layer_out = (residual.astype(jnp.float32) + mlp_sum).astype(jnp.bfloat16)
    widened_out = layer_out.astype(jnp.float32)
    row_check = lax.psum(jnp.sum(widened_out * widened_out, axis=1), "dp") / D
    return (layer_out, row_check)


MESH = pl.DeviceIdType.MESH
F32 = jnp.float32
BF16 = jnp.bfloat16


def fused(
    x_ref, kb_ref, gain_ref, wg_hbm, wu_hbm, wd_hbm, out_ref, chk_ref,
    wg, wu, wd, xbuf, xn, kw, kall, iown, iall, keep,
    pd, py, px, pown, relay, from_x, from_y, hbuf, qf, qb, sib, ssend, acc, zr, cown, call,
    w_sem, rx, tx_dp, tx_z, tx_s, rk, tk, ri, ti, rp, tp, rh, th, rs, ts, rz, tz, rc, tc,
):
    m, R = xbuf.shape[1], xbuf.shape[2]
    width = xbuf.shape[3]
    TB = m * R
    U = wg.shape[1]
    half_rows = out_ref.shape[0]
    words = kb_ref.shape[1] // m
    chips = m // 2
    tile = 256 if U % 256 == 0 and width % 256 == 0 else 128
    cut = (U // tile + 1) // 2 * tile
    parts = ((0, cut), (cut, U - cut))

    i, j = lax.axis_index("dp"), lax.axis_index("tensor")
    iy, ix = i // 2, i % 2
    z, c = j // 2, j % 2
    xnb = iy * 2 + (1 - ix)
    ynb = (1 - iy) * 2 + ix
    diag = (1 - iy) * 2 + (1 - ix)
    sibling = z * 2 + (1 - c)
    sends = []

    def send(src, dst, ss, rsem, to):
        copy = pltpu.make_async_remote_copy(
            src_ref=src, dst_ref=dst, send_sem=ss, recv_sem=rsem, device_id=to, device_id_type=MESH
        )
        copy.start()
        sends.append(copy)

    def arrived(dst, rsem):
        pltpu.make_async_remote_copy(
            src_ref=dst, dst_ref=dst, send_sem=tc.at[0], recv_sem=rsem,
            device_id=(i, sibling), device_id_type=MESH,
        ).wait_recv()

    loads = [pltpu.make_async_copy(s, d, w_sem.at[k]) for k, (s, d) in enumerate(((wg_hbm, wg), (wu_hbm, wu), (wd_hbm, wd)))]
    for load in loads:
        load.start()

    barrier = pltpu.get_barrier_semaphore()
    for other in (xnb, ynb, diag):
        pl.semaphore_signal(barrier, inc=1, device_id=(other, j), device_id_type=MESH)
    for step in range(1, m):
        pl.semaphore_signal(barrier, inc=1, device_id=(i, (j + step) % m), device_id_type=MESH)
    xbuf[i, j] = x_ref[:, pl.ds(pl.multiple_of(i * width, width), width)]
    pl.semaphore_wait(barrier, 3 + m - 1)

    for k, other in enumerate((diag, ynb, xnb)):
        send(x_ref.at[:, pl.ds(pl.multiple_of(other * width, width), width)], xbuf.at[i, j], tx_dp.at[k], rx.at[i, j], (other, j))

    kw[...] = jnp.zeros_like(kw)
    for t in range(m):
        kw[t, :, 0:words] = kb_ref[:, t * words : (t + 1) * words]
    rows = x_ref[...].astype(F32)
    total = jnp.sum(rows * rows, axis=1, keepdims=True)
    iown[...] = jnp.broadcast_to(lax.rsqrt(total / (x_ref.shape[1]) + 1e-05), iown.shape)
    iall[j] = iown[...]
    kall[j] = kw[j]

    order = (diag, ynb, xnb, i)
    for k, b in enumerate(order):
        if k < 3:
            arrived(xbuf.at[b, j], rx.at[b, j])
        for step in range(1, chips):
            to = ((z + step) % chips) * 2 + c
            send(xbuf.at[b, j], xbuf.at[b, j], tx_z.at[k, step - 1], rx.at[b, j], (i, to))
        send(xbuf.at[b, j], xbuf.at[b, j], tx_s.at[k, 0], rx.at[b, j], (i, sibling))
    for step in range(1, m):
        to = (j + step) % m
        send(kw.at[to], kall.at[j], tk.at[step - 1], rk.at[j], (i, to))
        send(iown, iall.at[j], ti.at[step - 1], ri.at[j], (i, to))

    gain = gain_ref[...].astype(F32)

    def collect(k):
        b = order[k]
        for step in range(1, chips):
            slot = ((z + step) % chips) * 2 + c
            arrived(xbuf.at[b, slot], rx.at[b, slot])
            send(xbuf.at[b, slot], xbuf.at[b, slot], tx_s.at[k, step], rx.at[b, slot], (i, sibling))
        for step in range(chips):
            slot = ((z + step) % chips) * 2 + (1 - c)
            arrived(xbuf.at[b, slot], rx.at[b, slot])

        def scale(t, carry):
            xn[k, pl.ds(pl.multiple_of(t * R, R), R), :] = (xbuf[b, t].astype(F32) * gain).astype(BF16)
            return carry

        lax.fori_loop(0, m, scale, 0)

    def project(k, w, dst, lo=0, hi=U, extra=None):
        def body(t, carry):
            cols = pl.ds(pl.multiple_of(t * tile, tile), tile)
            part = jnp.dot(xn[k], w[:, cols], preferred_element_type=F32)
            if extra is not None:
                part = part + extra[:, cols].astype(F32)
            dst[:, cols] = part.astype(dst.dtype)
            return carry

        lax.fori_loop(lo // tile, hi // tile, body, 0)

    collect(0)
    loads[0].wait()
    loads[1].wait()
    for p, (lo, size) in enumerate(parts):
        cols = pl.ds(lo, size)
        project(0, wg, pd.at[0], lo, lo + size)
        send(pd.at[0, :, cols], relay.at[0, :, cols], tp.at[p, 0], rp.at[p, 0], (xnb, j))
        project(0, wu, pd.at[1], lo, lo + size)
        send(pd.at[1, :, cols], relay.at[1, :, cols], tp.at[p, 1], rp.at[p, 1], (ynb, j))
        if p == 0:
            collect(1)
        project(1, wu, py.at[1], lo, lo + size)
        send(py.at[1, :, cols], from_y.at[1, :, cols], tp.at[p, 2], rp.at[p, 2], (ynb, j))
        if p == 0:
            collect(2)
        project(2, wg, px.at[0], lo, lo + size)
        send(px.at[0, :, cols], from_x.at[0, :, cols], tp.at[p, 3], rp.at[p, 3], (xnb, j))
        if p == 0:
            collect(3)
    for p, (lo, size) in enumerate(parts):
        cols = pl.ds(lo, size)
        arrived(relay.at[0, :, cols], rp.at[p, 0])
        project(1, wg, py.at[0], lo, lo + size, relay.at[0])
        send(py.at[0, :, cols], from_y.at[0, :, cols], tp.at[p, 4], rp.at[p, 4], (ynb, j))
        arrived(relay.at[1, :, cols], rp.at[p, 1])
        project(2, wu, px.at[1], lo, lo + size, relay.at[1])
        send(px.at[1, :, cols], from_x.at[1, :, cols], tp.at[p, 5], rp.at[p, 5], (xnb, j))
    project(3, wg, pown.at[0])
    project(3, wu, pown.at[1])

    for step in range(1, m):
        slot = (j + step) % m
        arrived(kall.at[slot], rk.at[slot])
        arrived(iall.at[slot], ri.at[slot])
    word = kall[...].reshape(TB, kall.shape[2])
    scale_rows = iall[...].reshape(TB, iall.shape[2])[:, 0:1]
    byte = [jnp.bitwise_and(jnp.right_shift(word, 8 * q), 255).astype(F32).astype(BF16) for q in range(4)]
    lanes = kall.shape[2]

    def expand(t, carry):
        unit = t * tile + lax.broadcasted_iota(jnp.int32, (lanes, tile), 1)
        where = lax.broadcasted_iota(jnp.int32, (lanes, tile), 0)
        spread = jnp.zeros((TB, tile), F32)
        for q in range(4):
            hit = (jnp.right_shift(unit, 3) == where * 4 + q)
            spread += jnp.dot(byte[q], jnp.where(hit, 1.0, 0.0).astype(BF16), preferred_element_type=F32)
        shift = jnp.bitwise_and(lax.broadcasted_iota(jnp.int32, (TB, tile), 1), 7)
        bit = jnp.bitwise_and(jnp.right_shift(spread.astype(jnp.int32), shift), 1)
        keep[:, pl.ds(pl.multiple_of(t * tile, tile), tile)] = (2 * bit).astype(F32)
        return carry

    lax.fori_loop(0, U // tile, expand, 0)

    for p, (lo, size) in enumerate(parts):
        cols = pl.ds(lo, size)
        arrived(from_y.at[1, :, cols], rp.at[p, 2])
        arrived(from_x.at[0, :, cols], rp.at[p, 3])
        arrived(from_y.at[0, :, cols], rp.at[p, 4])
        arrived(from_x.at[1, :, cols], rp.at[p, 5])

        def activate(t, carry):
            at = pl.ds(pl.multiple_of(t * tile, tile), tile)
            gate = (pown[0, :, at] + from_x[0, :, at].astype(F32) + from_y[0, :, at].astype(F32)) * scale_rows
            up = (pown[1, :, at] + from_x[1, :, at].astype(F32) + from_y[1, :, at].astype(F32)) * scale_rows
            hbuf[i, :, at] = (gate / (1.0 + jnp.exp(-gate)) * up * keep[:, at]).astype(BF16)
            return carry

        lax.fori_loop(lo // tile, (lo + size) // tile, activate, 0)
        send(hbuf.at[i, :, cols], hbuf.at[i, :, cols], th.at[p, 0], rh.at[i, p], (xnb, j))
        send(hbuf.at[i, :, cols], hbuf.at[i, :, cols], th.at[p, 1], rh.at[i, p], (ynb, j))

    loads[2].wait()
    blocks = (i, xnb, ynb, diag)

    def down(k):
        b = blocks[k]

        def body(t, carry):
            cols = pl.ds(pl.multiple_of(t * tile, tile), tile)
            part = jnp.dot(hbuf[b], wd[:, cols], preferred_element_type=F32)
            for h in range(2):
                piece = part[h * half_rows : (h + 1) * half_rows]
                qf[k, h, :, cols] = piece
                qb[k, h, :, cols] = piece.astype(BF16)
            return carry

        lax.fori_loop(0, width // tile, body, 0)
        send(qb.at[k, 1 - c], sib.at[k], ts.at[k], rs.at[k], (i, sibling))

    z_sends = []

    def pair(k):
        b = blocks[k]
        arrived(sib.at[k], rs.at[k])
        both = qf[k, c] + sib[k].astype(F32)
        copy = pltpu.make_async_remote_copy(
            src_ref=ssend.at[k], dst_ref=zr.at[z], send_sem=tz.at[k], recv_sem=rz.at[z],
            device_id=(i, b * 2 + c), device_id_type=MESH,
        )

        @pl.when(b == z)
        def _():
            acc[...] = both

        @pl.when(b != z)
        def _():
            ssend[k] = both.astype(BF16)
            copy.start()

        z_sends.append((b, copy))

    down(0)
    p0, p1 = (pl.ds(lo, size) for lo, size in parts)
    arrived(hbuf.at[xnb, :, p0], rh.at[xnb, 0])
    send(hbuf.at[xnb, :, p0], hbuf.at[xnb, :, p0], th.at[0, 2], rh.at[xnb, 0], (ynb, j))
    pair(0)
    arrived(hbuf.at[ynb, :, p0], rh.at[ynb, 0])
    arrived(hbuf.at[ynb, :, p1], rh.at[ynb, 1])
    send(hbuf.at[ynb, :, p1], hbuf.at[ynb, :, p1], th.at[1, 2], rh.at[ynb, 1], (xnb, j))
    arrived(hbuf.at[xnb, :, p1], rh.at[xnb, 1])
    down(1)
    down(2)
    pair(1)
    pair(2)
    arrived(hbuf.at[diag, :, p0], rh.at[diag, 0])
    arrived(hbuf.at[diag, :, p1], rh.at[diag, 1])
    down(3)
    pair(3)

    first = j * (half_rows // R)
    mine = xbuf.reshape(xbuf.shape[0] * m, R, width)
    value = acc[...]
    for step in range(1, chips):
        slot = (z + step) % chips
        arrived(zr.at[slot], rz.at[slot])
        value = value + zr[slot].astype(F32)
    acc[...] = value
    sums = []
    for q in range(half_rows // R):
        rows_q = pl.ds(q * R, R)
        result = (mine[first + q].astype(F32) + acc[rows_q, :]).astype(BF16)
        out_ref[rows_q, :] = result
        wide = result.astype(F32)
        cown[rows_q, :] = jnp.broadcast_to(jnp.sum(wide * wide, axis=1, keepdims=True), (R, cown.shape[1]))
    for k, other in enumerate((xnb, ynb, diag)):
        send(cown, call.at[i], tc.at[k], rc.at[i], (other, j))
    check = cown[...]
    for other in (xnb, ynb, diag):
        arrived(call.at[other], rc.at[other])
        check = check + call[other]
    chk_ref[...] = check / x_ref.shape[1]

    for copy in sends:
        copy.wait_send()
    for b, copy in z_sends:

        @pl.when(b != z)
        def _():
            copy.wait_send()


def on_plane(saved_input, keep_bits, norm_gain, gate_weight, up_weight, down_weight):
    n, m = lax.axis_size("dp"), lax.axis_size("tensor")
    R, full = saved_input.shape
    width, U = gate_weight.shape
    TB = R * m
    out_rows = n * TB // m
    chips = m // 2
    lanes = -(-(keep_bits.shape[1] // m) // 128) * 128
    dma = pltpu.SemaphoreType.DMA
    vmem = pl.BlockSpec(memory_space=pltpu.VMEM)
    hbm = pl.BlockSpec(memory_space=pl.ANY)
    scratch = [
        pltpu.VMEM((width, U), BF16), pltpu.VMEM((width, U), BF16), pltpu.VMEM((U, width), BF16),
        pltpu.VMEM((n, m, R, width), BF16), pltpu.VMEM((n, TB, width), BF16),
        pltpu.VMEM((m, R, lanes), jnp.int32), pltpu.VMEM((m, R, lanes), jnp.int32),
        pltpu.VMEM((R, 128), F32), pltpu.VMEM((m, R, 128), F32), pltpu.VMEM((TB, U), F32),
        pltpu.VMEM((2, TB, U), BF16), pltpu.VMEM((2, TB, U), BF16), pltpu.VMEM((2, TB, U), BF16),
        pltpu.VMEM((2, TB, U), F32), pltpu.VMEM((2, TB, U), BF16),
        pltpu.VMEM((2, TB, U), BF16), pltpu.VMEM((2, TB, U), BF16),
        pltpu.VMEM((n, TB, U), BF16),
        pltpu.VMEM((n, 2, out_rows, width), F32), pltpu.VMEM((n, 2, out_rows, width), BF16),
        pltpu.VMEM((n, out_rows, width), BF16), pltpu.VMEM((n, out_rows, width), BF16),
        pltpu.VMEM((out_rows, width), F32), pltpu.VMEM((chips, out_rows, width), BF16),
        pltpu.VMEM((out_rows, 128), F32), pltpu.VMEM((n, out_rows, 128), F32),
        dma((3,)), dma((n, m)), dma((3,)), dma((n, chips - 1)), dma((n, chips)),
        dma((m,)), dma((m - 1,)), dma((m,)), dma((m - 1,)),
        dma((2, 6)), dma((2, 6)), dma((n, 2)), dma((2, 3)),
        dma((n,)), dma((n,)), dma((chips,)), dma((n,)), dma((n,)), dma((3,)),
    ]
    layer_out, check = pl.pallas_call(
        fused,
        out_shape=(
            jax.ShapeDtypeStruct((out_rows, width), BF16),
            jax.ShapeDtypeStruct((out_rows, 128), F32),
        ),
        in_specs=[vmem, vmem, vmem, hbm, hbm, hbm],
        out_specs=(vmem, vmem),
        scratch_shapes=scratch,
        compiler_params=pltpu.CompilerParams(
            collective_id=0, has_side_effects=True, vmem_limit_bytes=60 * 1024 * 1024
        ),
    )(saved_input, keep_bits, norm_gain.reshape(1, width), gate_weight, up_weight, down_weight)
    return layer_out, check[:, 0]


def solution(mesh):
    placed = (
        P(("dp", "tensor"), None),
        P(("dp", "tensor"), None),
        P("dp"),
        P("dp", "tensor"),
        P("dp", "tensor"),
        P("tensor", "dp"),
    )
    plane = mesh.shape["dp"] == 4 and mesh.shape["tensor"] == 2 * mesh.shape["dp"]
    return jax.shard_map(
        on_plane if plane else on_device,
        mesh=mesh,
        in_specs=placed,
        out_specs=(P("tensor", "dp"), P("tensor")),
        check_vma=False,
    )
```

```python
import jax
import jax.numpy as jnp
from jax import lax
from jax.experimental import pallas as pl
from jax.experimental.pallas import tpu as pltpu
from jax.sharding import PartitionSpec as P

D = 8192


def on_device(saved_input, keep_bits, norm_gain, gate_weight, up_weight, down_weight):
    tensor_width = lax.axis_size("tensor")
    dp_width = lax.axis_size("dp")
    unit_words = lax.all_to_all(keep_bits, "tensor", split_axis=1, concat_axis=0, tiled=True)
    shifts = jnp.arange(32, dtype=jnp.int32)
    keep_mask = jnp.bitwise_and(jnp.right_shift(unit_words[:, :, None], shifts[None, None, :]), 1)
    keep_mask = keep_mask.reshape(unit_words.shape[0], -1)
    keep_scale = 2.0 * keep_mask.astype(jnp.float32)
    width_units = gate_weight.shape[1]
    columns = lax.all_to_all(saved_input, "dp", split_axis=1, concat_axis=0, tiled=True)
    collected = lax.all_gather(columns, "tensor", axis=0, tiled=True)
    per_device = saved_input.shape[0]
    collected = collected.reshape(tensor_width, dp_width, per_device, collected.shape[1])
    collected = collected.transpose(1, 0, 2, 3).reshape(-1, collected.shape[3])
    widened = collected.astype(jnp.float32)
    squares = lax.psum(jnp.sum(widened * widened, axis=1), "dp")
    inv_rms = lax.rsqrt(squares / D + 1e-05)
    normed = (widened * inv_rms[:, None] * norm_gain.astype(jnp.float32)[None, :]).astype(
        jnp.bfloat16
    )
    gate_part = jnp.dot(normed, gate_weight, preferred_element_type=jnp.float32)
    up_part = jnp.dot(normed, up_weight, preferred_element_type=jnp.float32)
    projected = lax.psum_scatter(
        jnp.concatenate((gate_part, up_part), axis=1).astype(jnp.bfloat16),
        "dp",
        scatter_dimension=0,
        tiled=True,
    ).astype(jnp.float32)
    gate_sum = projected[:, :width_units]
    up_sum = projected[:, width_units:]
    hidden = (jax.nn.silu(gate_sum) * up_sum * keep_scale).astype(jnp.bfloat16)
    partial_value = jnp.dot(
        lax.all_gather(hidden, "dp", axis=0, tiled=True),
        down_weight,
        preferred_element_type=jnp.float32,
    )
    mlp_sum = lax.psum_scatter(
        partial_value.astype(jnp.bfloat16), "tensor", scatter_dimension=0, tiled=True
    ).astype(jnp.float32)
    out_rows = mlp_sum.shape[0]
    first_row = lax.axis_index("tensor") * out_rows
    residual = lax.dynamic_slice_in_dim(collected, first_row, out_rows, 0)
    layer_out = (residual.astype(jnp.float32) + mlp_sum).astype(jnp.bfloat16)
    widened_out = layer_out.astype(jnp.float32)
    row_check = lax.psum(jnp.sum(widened_out * widened_out, axis=1), "dp") / D
    return (layer_out, row_check)


MESH = pl.DeviceIdType.MESH
F32 = jnp.float32
BF16 = jnp.bfloat16
COL_PARTS = 4


def fused(
    x_ref, kb_ref, gain_ref, wg_hbm, wu_hbm, wd_hbm, out_ref, chk_ref,
    wg, wu, wd, xbuf, xn, kw, kall, iown, iall, keep,
    pd, py, px, pown, relay, from_x, from_y, hbuf, qf, qb, sib, ssend, acc, zr, zpass, cown, call,
    w_sem, rx, tx_dp, tx_z, tx_s, rk, tk, ri, ti, rp, tp, rh, th, rs, ts, rz, rpass, tz, rc, tc,
):
    m, R = xbuf.shape[1], xbuf.shape[2]
    width = xbuf.shape[3]
    TB = m * R
    U = wg.shape[1]
    half_rows = out_ref.shape[0]
    words = kb_ref.shape[1] // m
    tile = 256 if U % 256 == 0 and width % 256 == 0 else 128
    step_cols = -(-(U // tile) // COL_PARTS) * tile
    parts = tuple((lo, min(step_cols, U - lo)) for lo in range(0, U, step_cols))

    i, j = lax.axis_index("dp"), lax.axis_index("tensor")
    iy, ix = i // 2, i % 2
    z, c = j // 2, j % 2
    xnb = iy * 2 + (1 - ix)
    ynb = (1 - iy) * 2 + ix
    diag = (1 - iy) * 2 + (1 - ix)
    sibling = z * 2 + (1 - c)
    mate = z + 1 - 2 * (z % 2)
    far, far_end = 2 - z // 2, 3 * (1 - z // 2)
    inner = (z + 1) // 2 == 1
    sends, inner_sends = [], []

    def send(src, dst, ss, rsem, to):
        copy = pltpu.make_async_remote_copy(
            src_ref=src, dst_ref=dst, send_sem=ss, recv_sem=rsem, device_id=to, device_id_type=MESH
        )
        copy.start()
        sends.append(copy)

    def arrived(dst, rsem):
        pltpu.make_async_remote_copy(
            src_ref=dst, dst_ref=dst, send_sem=tc.at[0], recv_sem=rsem,
            device_id=(i, sibling), device_id_type=MESH,
        ).wait_recv()

    loads = [pltpu.make_async_copy(s, d, w_sem.at[k]) for k, (s, d) in enumerate(((wg_hbm, wg), (wu_hbm, wu), (wd_hbm, wd)))]
    for load in loads:
        load.start()

    barrier = pltpu.get_barrier_semaphore()
    for other in (xnb, ynb, diag):
        pl.semaphore_signal(barrier, inc=1, device_id=(other, j), device_id_type=MESH)
    for step in range(1, m):
        pl.semaphore_signal(barrier, inc=1, device_id=(i, (j + step) % m), device_id_type=MESH)
    xbuf[i, j] = x_ref[:, pl.ds(pl.multiple_of(i * width, width), width)]
    pl.semaphore_wait(barrier, 3 + m - 1)

    for k, other in enumerate((diag, ynb, xnb)):
        send(x_ref.at[:, pl.ds(pl.multiple_of(other * width, width), width)], xbuf.at[i, j], tx_dp.at[k], rx.at[i, j], (other, j))

    kw[...] = jnp.zeros_like(kw)
    for t in range(m):
        kw[t, :, 0:words] = kb_ref[:, t * words : (t + 1) * words]
    rows = x_ref[...].astype(F32)
    total = jnp.sum(rows * rows, axis=1, keepdims=True)
    iown[...] = jnp.broadcast_to(lax.rsqrt(total / (x_ref.shape[1]) + 1e-05), iown.shape)
    iall[j] = iown[...]
    kall[j] = kw[j]

    order = (diag, ynb, xnb, i)
    for k, b in enumerate(order):
        if k < 3:
            arrived(xbuf.at[b, j], rx.at[b, j])
        for q, to in enumerate((mate, far)):
            send(xbuf.at[b, j], xbuf.at[b, j], tx_z.at[k, q], rx.at[b, j], (i, to * 2 + c))
        send(xbuf.at[b, j], xbuf.at[b, j], tx_s.at[k, 0], rx.at[b, j], (i, sibling))

    gain = gain_ref[...].astype(F32).reshape(1, width)

    def forward(k):
        b = order[k]
        for q, chip in enumerate((mate, far, far_end)):
            slot = chip * 2 + c
            arrived(xbuf.at[b, slot], rx.at[b, slot])
            if q > 0:
                copy = pltpu.make_async_remote_copy(
                    src_ref=xbuf.at[b, slot], dst_ref=xbuf.at[b, slot], send_sem=tx_z.at[k, q + 1],
                    recv_sem=rx.at[b, slot], device_id=(i, mate * 2 + c), device_id_type=MESH,
                )
                pl.when(inner)(copy.start)
                inner_sends.append(copy)
            send(xbuf.at[b, slot], xbuf.at[b, slot], tx_s.at[k, q + 1], rx.at[b, slot], (i, sibling))

    def collect(k):
        b = order[k]
        for chip in (z, mate, far, far_end):
            slot = chip * 2 + (1 - c)
            arrived(xbuf.at[b, slot], rx.at[b, slot])

        def scale(t, carry):
            xn[k, pl.ds(pl.multiple_of(t * R, R), R), :] = (xbuf[b, t].astype(F32) * gain).astype(BF16)
            return carry

        lax.fori_loop(0, m, scale, 0)

    def project(k, w, dst, lo=0, hi=U, extra=None):
        def body(t, carry):
            cols = pl.ds(pl.multiple_of(t * tile, tile), tile)
            part = jnp.dot(xn[k], w[:, cols], preferred_element_type=F32)
            if extra is not None:
                part = part + extra[:, cols].astype(F32)
            dst[:, cols] = part.astype(dst.dtype)
            return carry

        lax.fori_loop(lo // tile, hi // tile, body, 0)

    def stage(k, w, dst, to, land, slot):
        for p, (lo, size) in enumerate(parts):
            cols = pl.ds(lo, size)
            project(k, w, dst, lo, lo + size)
            send(dst.at[:, cols], land.at[:, cols], tp.at[p, slot], rp.at[p, slot], (to, j))

    forward(0)
    collect(0)
    loads[0].wait()
    loads[1].wait()
    for p, (lo, size) in enumerate(parts):
        cols = pl.ds(lo, size)
        project(0, wg, pd.at[0], lo, lo + size)
        send(pd.at[0, :, cols], relay.at[0, :, cols], tp.at[p, 0], rp.at[p, 0], (xnb, j))
        project(0, wu, pd.at[1], lo, lo + size)
        send(pd.at[1, :, cols], relay.at[1, :, cols], tp.at[p, 1], rp.at[p, 1], (ynb, j))
    forward(1)
    collect(1)
    stage(1, wu, py.at[1], ynb, from_y.at[1], 2)
    forward(2)
    collect(2)
    stage(2, wg, px.at[0], xnb, from_x.at[0], 3)
    forward(3)
    for p, (lo, size) in enumerate(parts):
        cols = pl.ds(lo, size)
        arrived(relay.at[0, :, cols], rp.at[p, 0])
        project(1, wg, py.at[0], lo, lo + size, relay.at[0])
        send(py.at[0, :, cols], from_y.at[0, :, cols], tp.at[p, 4], rp.at[p, 4], (ynb, j))
        arrived(relay.at[1, :, cols], rp.at[p, 1])
        project(2, wu, px.at[1], lo, lo + size, relay.at[1])
        send(px.at[1, :, cols], from_x.at[1, :, cols], tp.at[p, 5], rp.at[p, 5], (xnb, j))
    for step in range(1, m):
        to = (j + step) % m
        send(kw.at[to], kall.at[j], tk.at[step - 1], rk.at[j], (i, to))
        send(iown, iall.at[j], ti.at[step - 1], ri.at[j], (i, to))
    collect(3)
    project(3, wg, pown.at[0])
    project(3, wu, pown.at[1])

    for step in range(1, m):
        slot = (j + step) % m
        arrived(kall.at[slot], rk.at[slot])
        arrived(iall.at[slot], ri.at[slot])
    word = kall[...].reshape(TB, kall.shape[2])
    scale_rows = iall[...].reshape(TB, iall.shape[2])[:, 0:1]
    byte = [jnp.bitwise_and(jnp.right_shift(word, 8 * q), 255).astype(F32).astype(BF16) for q in range(4)]
    lanes = kall.shape[2]

    def expand(t, carry):
        unit = t * tile + lax.broadcasted_iota(jnp.int32, (lanes, tile), 1)
        where = lax.broadcasted_iota(jnp.int32, (lanes, tile), 0)
        spread = jnp.zeros((TB, tile), F32)
        for q in range(4):
            hit = (jnp.right_shift(unit, 3) == where * 4 + q)
            spread += jnp.dot(byte[q], jnp.where(hit, 1.0, 0.0).astype(BF16), preferred_element_type=F32)
        shift = jnp.bitwise_and(lax.broadcasted_iota(jnp.int32, (TB, tile), 1), 7)
        bit = jnp.bitwise_and(jnp.right_shift(spread.astype(jnp.int32), shift), 1)
        keep[:, pl.ds(pl.multiple_of(t * tile, tile), tile)] = (2 * bit).astype(F32)
        return carry

    lax.fori_loop(0, U // tile, expand, 0)

    for p, (lo, size) in enumerate(parts):
        cols = pl.ds(lo, size)
        arrived(from_y.at[1, :, cols], rp.at[p, 2])
        arrived(from_x.at[0, :, cols], rp.at[p, 3])
        arrived(from_y.at[0, :, cols], rp.at[p, 4])
        arrived(from_x.at[1, :, cols], rp.at[p, 5])

        def activate(t, carry):
            at = pl.ds(pl.multiple_of(t * tile, tile), tile)
            gate = (pown[0, :, at] + from_x[0, :, at].astype(F32) + from_y[0, :, at].astype(F32)) * scale_rows
            up = (pown[1, :, at] + from_x[1, :, at].astype(F32) + from_y[1, :, at].astype(F32)) * scale_rows
            hbuf[i, :, at] = (gate / (1.0 + jnp.exp(-gate)) * up * keep[:, at]).astype(BF16)
            return carry

        lax.fori_loop(lo // tile, (lo + size) // tile, activate, 0)
        send(hbuf.at[i, :, cols], hbuf.at[i, :, cols], th.at[p, 0], rh.at[i, p], (xnb, j))
        send(hbuf.at[i, :, cols], hbuf.at[i, :, cols], th.at[p, 1], rh.at[i, p], (ynb, j))

    loads[2].wait()
    blocks = (i, xnb, ynb, diag)

    span = width // 2
    halves = [pl.ds(h * span, span) for h in range(2)]

    def down(k, h):
        b = blocks[k]

        def body(t, carry):
            cols = pl.ds(pl.multiple_of(t * tile, tile), tile)
            part = jnp.dot(hbuf[b], wd[:, cols], preferred_element_type=F32)
            for r in range(2):
                piece = part[r * half_rows : (r + 1) * half_rows]
                qf[k, r, :, cols] = piece
                qb[k, r, :, cols] = piece.astype(BF16)
            return carry

        lax.fori_loop(h * span // tile, (h + 1) * span // tile, body, 0)
        at = halves[h]
        send(qb.at[k, 1 - c, :, at], sib.at[k, :, at], ts.at[k, h], rs.at[k, h], (i, sibling))

    away_sends = []

    def pair(k, h):
        b, at = blocks[k], halves[h]
        arrived(sib.at[k, :, at], rs.at[k, h])
        qf[k, c, :, at] = qf[k, c, :, at] + sib[k, :, at].astype(F32)
        here, near = b == z, b == mate
        away = b // 2 != z // 2
        outer = (z + 1) // 2 != 1

        def copy_to(dst, rsem, chip):
            return pltpu.make_async_remote_copy(
                src_ref=ssend.at[k, :, at], dst_ref=dst, send_sem=tz.at[k, h], recv_sem=rsem,
                device_id=(i, chip * 2 + c), device_id_type=MESH,
            )

        direct = copy_to(zr.at[0, :, at], rz.at[0, h], mate)
        passed = copy_to(zpass.at[b, :, at], rpass.at[b, h], mate)
        joined = copy_to(zr.at[1, :, at], rz.at[1, h], b)

        @pl.when(here)
        def _():
            acc[:, at] = qf[k, c, :, at]

        @pl.when(near)
        def _():
            ssend[k, :, at] = qf[k, c, :, at].astype(BF16)
            direct.start()

        @pl.when(jnp.logical_and(away, outer))
        def _():
            ssend[k, :, at] = qf[k, c, :, at].astype(BF16)
            passed.start()

        away_sends.append((here, away, direct, joined))

    def join(k, h):
        b, at = blocks[k], halves[h]
        _, away, _, joined = away_sends[2 * k + h]

        @pl.when(jnp.logical_and(away, inner))
        def _():
            arrived(zpass.at[b, :, at], rpass.at[b, h])
            ssend[k, :, at] = (qf[k, c, :, at] + zpass[b, :, at].astype(F32)).astype(BF16)
            joined.start()

    def hand_on(p):
        cols = pl.ds(parts[p][0], parts[p][1])
        src, to = ((xnb, ynb), (ynb, xnb))[p % 2]
        arrived(hbuf.at[src, :, cols], rh.at[src, p])
        send(hbuf.at[src, :, cols], hbuf.at[src, :, cols], th.at[p, 2], rh.at[src, p], (to, j))

    def rest(p, src):
        cols = pl.ds(parts[p][0], parts[p][1])
        arrived(hbuf.at[src, :, cols], rh.at[src, p])

    last = len(parts) - 1
    down(0, 0)
    hand_on(0)
    down(0, 1)
    pair(0, 0)
    for p in range(1, last):
        hand_on(p)
    pair(0, 1)
    hand_on(last)
    for p in range(1, last + 1, 2):
        rest(p, xnb)
    down(1, 0)
    down(1, 1)
    pair(1, 0)
    for p in range(0, last + 1, 2):
        rest(p, ynb)
    down(2, 0)
    pair(1, 1)
    join(0, 0)
    join(0, 1)
    down(2, 1)
    pair(2, 0)
    for p in range(last + 1):
        rest(p, diag)
    down(3, 0)
    pair(2, 1)
    down(3, 1)
    pair(3, 0)
    pair(3, 1)
    for k in range(1, 4):
        join(k, 0)
        join(k, 1)

    first = j * (half_rows // R)
    mine = xbuf.reshape(xbuf.shape[0] * m, R, width)
    value = acc[...]
    for slot in range(2):
        for h in range(2):
            arrived(zr.at[slot, :, halves[h]], rz.at[slot, h])
        value = value + zr[slot].astype(F32)
    acc[...] = value
    sums = []
    for q in range(half_rows // R):
        rows_q = pl.ds(q * R, R)
        result = (mine[first + q].astype(F32) + acc[rows_q, :]).astype(BF16)
        out_ref[rows_q, :] = result
        wide = result.astype(F32)
        cown[rows_q, :] = jnp.broadcast_to(jnp.sum(wide * wide, axis=1, keepdims=True), (R, cown.shape[1]))
    for k, other in enumerate((xnb, ynb, diag)):
        send(cown, call.at[i], tc.at[k], rc.at[i], (other, j))
    check = cown[...]
    for other in (xnb, ynb, diag):
        arrived(call.at[other], rc.at[other])
        check = check + call[other]
    chk_ref[...] = jnp.transpose(check / x_ref.shape[1])[0]

    for copy in sends:
        copy.wait_send()
    for copy in inner_sends:
        pl.when(inner)(copy.wait_send)
    for here, _, copy, _ in away_sends:
        pl.when(jnp.logical_not(here))(copy.wait_send)


def on_plane(saved_input, keep_bits, norm_gain, gate_weight, up_weight, down_weight):
    n, m = lax.axis_size("dp"), lax.axis_size("tensor")
    R, full = saved_input.shape
    width, U = gate_weight.shape
    TB = R * m
    out_rows = n * TB // m
    chips = m // 2
    lanes = -(-(keep_bits.shape[1] // m) // 128) * 128
    dma = pltpu.SemaphoreType.DMA
    vmem = pl.BlockSpec(memory_space=pltpu.VMEM)
    hbm = pl.BlockSpec(memory_space=pl.ANY)
    scratch = [
        pltpu.VMEM((width, U), BF16), pltpu.VMEM((width, U), BF16), pltpu.VMEM((U, width), BF16),
        pltpu.VMEM((n, m, R, width), BF16), pltpu.VMEM((n, TB, width), BF16),
        pltpu.VMEM((m, R, lanes), jnp.int32), pltpu.VMEM((m, R, lanes), jnp.int32),
        pltpu.VMEM((R, 128), F32), pltpu.VMEM((m, R, 128), F32), pltpu.VMEM((TB, U), F32),
        pltpu.VMEM((2, TB, U), BF16), pltpu.VMEM((2, TB, U), BF16), pltpu.VMEM((2, TB, U), BF16),
        pltpu.VMEM((2, TB, U), F32), pltpu.VMEM((2, TB, U), BF16),
        pltpu.VMEM((2, TB, U), BF16), pltpu.VMEM((2, TB, U), BF16),
        pltpu.VMEM((n, TB, U), BF16),
        pltpu.VMEM((n, 2, out_rows, width), F32), pltpu.VMEM((n, 2, out_rows, width), BF16),
        pltpu.VMEM((n, out_rows, width), BF16), pltpu.VMEM((n, out_rows, width), BF16),
        pltpu.VMEM((out_rows, width), F32), pltpu.VMEM((2, out_rows, width), BF16), pltpu.VMEM((n, out_rows, width), BF16),
        pltpu.VMEM((out_rows, 128), F32), pltpu.VMEM((n, out_rows, 128), F32),
        dma((3,)), dma((n, m)), dma((3,)), dma((n, 4)), dma((n, chips)),
        dma((m,)), dma((m - 1,)), dma((m,)), dma((m - 1,)),
        dma((COL_PARTS, 6)), dma((COL_PARTS, 6)), dma((n, COL_PARTS)), dma((COL_PARTS, 3)),
        dma((n, 2)), dma((n, 2)), dma((2, 2)), dma((n, 2)), dma((n, 2)), dma((n,)), dma((3,)),
    ]
    layer_out, check = pl.pallas_call(
        fused,
        out_shape=(
            jax.ShapeDtypeStruct((out_rows, width), BF16),
            jax.ShapeDtypeStruct((out_rows,), F32),
        ),
        in_specs=[vmem, vmem, vmem, hbm, hbm, hbm],
        out_specs=(vmem, vmem),
        scratch_shapes=scratch,
        compiler_params=pltpu.CompilerParams(
            collective_id=0, has_side_effects=True, vmem_limit_bytes=60 * 1024 * 1024
        ),
    )(saved_input, keep_bits, norm_gain, gate_weight, up_weight, down_weight)
    return layer_out, check


def solution(mesh):
    placed = (
        P(("dp", "tensor"), None),
        P(("dp", "tensor"), None),
        P("dp"),
        P("dp", "tensor"),
        P("dp", "tensor"),
        P("tensor", "dp"),
    )
    plane = mesh.shape["dp"] == 4 and mesh.shape["tensor"] == 2 * mesh.shape["dp"]
    return jax.shard_map(
        on_plane if plane else on_device,
        mesh=mesh,
        in_specs=placed,
        out_specs=(P("tensor", "dp"), P("tensor")),
        check_vma=False,
    )
```
